64 devices in a mesh: pod: 4 (over x, y), mp: 16 (over z, core).
Axes of the slice: x: 2, y: 2, z: 8, core: 2. Of those that a mesh axis runs over, the one named last changes fastest.
The devices are a block of a 4x4x8 slice.
Arguments:
- d_pool: bfloat16 [131072, 26, 128], P(('pod', 'mp')), parts along dimension 0
- row_ids: int32 [128, 32768, 1], P(('pod', 'mp')), parts along dimension 0
- lengths: int32 [128, 32768], P(('pod', 'mp')), parts along dimension 0
- tables: bfloat16 [128, 8192, 128], P(('pod', 'mp')), parts along dimension 0
- row_accum: float32 [128, 8192], P(('pod', 'mp')), parts along dimension 0
- learn_rate: float32 [], replicated
Outputs:
- output 1: bfloat16 [128, 8192, 128], P(('pod', 'mp')), parts along dimension 0
- output 2: float32 [128, 8192], P(('pod', 'mp')), parts along dimension 0
There are 4 independent parts. The reference program is written for one: setup_inputs(seed, part) draws one part's arguments, and reference() takes and returns one part's arrays. A program takes and returns all parts, laid end to end along the dimension named above; an argument that names none is the same for every part.
All inputs are finite; a program needn't handle non-finite values.
Results may differ from the reference program's by a relative error of at most 0.001.
Values are sent between devices in bfloat16 or wider.
A program may use at most 768 MiB of HBM per device.

```python
import jax
import jax.numpy as jnp
from jax import lax

TABLES = 26
EMB_DIM = 128
TABLE_ROWS = 8192
MAX_HOT = 1
N_SLOTS = 32
BATCH_ALL = 32768
HOT_SET = 64
EPSILON = 1e-06
HOTNESS_LIST = (3, 2, 1, 2, 6, 1, 1, 1, 1, 7, 3, 8, 1, 6, 9, 5, 1, 1, 1, 12, 100, 27, 10, 3, 1, 1)


def slot_hotness():
    hot_list = [min(HOTNESS_LIST[table_idx], MAX_HOT) if table_idx < TABLES else 0 for table_idx in range(N_SLOTS)]
    return jnp.array(hot_list, dtype=jnp.int32)


def draw_routing(route_key):
    slot_hot = slot_hotness()[:, None]
    key_len, key_pick, key_hot, key_uni = jax.random.split(route_key, 4)
    id_shape = (N_SLOTS, BATCH_ALL, MAX_HOT)
    raw_len = jax.random.randint(key_len, (N_SLOTS, BATCH_ALL), 0, 1 << 20)
    lengths = jnp.where(slot_hot > 0, raw_len % (slot_hot + 1), 0)
    lengths = lengths.at[:, 0].set(slot_hot[:, 0])
    hot_pick = jax.random.randint(key_pick, id_shape, 0, 4)
    hot_ids = jax.random.randint(key_hot, id_shape, 0, HOT_SET) * (TABLE_ROWS // HOT_SET)
    uni_ids = jax.random.randint(key_uni, id_shape, 0, TABLE_ROWS)
    row_ids = jnp.where(hot_pick == 0, hot_ids, uni_ids)
    row_ids = row_ids.at[:, 0, 0].set(TABLE_ROWS - 1)
    row_ids = row_ids.at[:, 1, 0].set(0)
    return row_ids.astype(jnp.int32), lengths.astype(jnp.int32)


def setup_inputs(seed: int = 0, part: int = 0) -> dict:
    seed_key = jax.random.key(seed)
    part_key = jax.random.fold_in(seed_key, part)
    key_grad, key_tab, key_acc, key_route = jax.random.split(part_key, 4)
    d_pool = jax.random.normal(key_grad, (BATCH_ALL, TABLES, EMB_DIM), jnp.float32).astype(jnp.bfloat16)
    row_ids, lengths = draw_routing(key_route)
    tables = jax.random.normal(key_tab, (N_SLOTS, TABLE_ROWS, EMB_DIM), jnp.float32).astype(jnp.bfloat16)
    row_accum = jax.random.uniform(key_acc, (N_SLOTS, TABLE_ROWS), jnp.float32, 0.2, 1.0)
    learn_rate = jax.random.uniform(jax.random.key(seed + 1), (), jnp.float32, 0.5, 1.5)
    return {'d_pool': d_pool, 'row_ids': row_ids, 'lengths': lengths, 'tables': tables, 'row_accum': row_accum, 'learn_rate': learn_rate}


def reference(d_pool, row_ids, lengths, tables, row_accum, learn_rate):
    padded = jnp.pad(d_pool, ((0, 0), (0, N_SLOTS - TABLES), (0, 0)))
    by_slot = jnp.transpose(padded, (1, 0, 2))
    positions = jnp.arange(MAX_HOT)

    def one_slot(packed):
        slot_grad, slot_ids, slot_len, slot_table, slot_accum = packed
        grad_vals = slot_grad.astype(jnp.float32)

        def add_position(row_grad, pos_idx):
            keep_mask = (pos_idx < slot_len)[:, None]
            row_grad = row_grad.at[slot_ids[:, pos_idx]].add(jnp.where(keep_mask, grad_vals, 0.0))
            return row_grad, None

        row_grad, unused_out = lax.scan(add_position, jnp.zeros((TABLE_ROWS, EMB_DIM), jnp.float32), positions)
        new_accum = slot_accum + jnp.mean(row_grad * row_grad, axis=-1)
        row_scale = learn_rate / (jnp.sqrt(new_accum) + EPSILON)
        new_table = (slot_table.astype(jnp.float32) - row_grad * row_scale[:, None]).astype(jnp.bfloat16)
        return new_table, new_accum

    new_tables, new_accum = lax.map(one_slot, (by_slot, row_ids, lengths, tables, row_accum))
    return new_tables, new_accum
```

```python
import functools

import jax
import jax.numpy as jnp
from jax import lax
from jax.experimental import pallas as pl
from jax.experimental.pallas import tpu as pltpu
from jax.sharding import PartitionSpec as P

EPSILON = 1e-06
SUB = 256
COPIES = 8
ROWS = 16


def compact_kernel(cap, start_ref, len_ref, grad_ref, out_ref, rows_ref):
    table = pl.program_id(0)
    n_sub = len_ref.shape[1]
    valid = len_ref[0]
    before = lax.broadcasted_iota(jnp.int32, (SUB, SUB), 0) < lax.broadcasted_iota(jnp.int32, (SUB, SUB), 1)
    rank = jnp.dot(valid.astype(jnp.bfloat16), before.astype(jnp.bfloat16), preferred_element_type=jnp.float32)
    rank = jnp.where(valid > 0, rank, -1.0)
    place = lax.broadcasted_iota(jnp.int32, (SUB, SUB), 0).astype(jnp.float32)
    for sub in range(n_sub):
        pick = jnp.where(place == rank[sub : sub + 1, :], 1.0, 0.0).astype(jnp.bfloat16)
        moved = jnp.dot(pick, grad_ref[0, sub * SUB : (sub + 1) * SUB, :], preferred_element_type=jnp.float32)
        rows_ref[pl.ds(start_ref[table, sub], SUB), :] = moved
    out_ref[0] = rows_ref[:cap, :].astype(jnp.bfloat16)


def compact_rows(by_table, lens, starts, half, cap, n_group):
    n_tab, batch, emb = by_table.shape
    n_half = (n_tab - half + 1) // 2
    return pl.pallas_call(
        functools.partial(compact_kernel, cap),
        grid=(n_half,),
        in_specs=[
            pl.BlockSpec(memory_space=pltpu.SMEM),
            pl.BlockSpec((1,) + lens.shape[1:], lambda i: (2 * i + half, 0, 0)),
            pl.BlockSpec((1, batch, emb), lambda i: (2 * i + half, 0, 0)),
        ],
        out_specs=pl.BlockSpec((1, cap, emb), lambda i: (i, 0, 0)),
        out_shape=jax.ShapeDtypeStruct((n_group, cap, emb), jnp.bfloat16),
        scratch_shapes=[pltpu.VMEM((batch + SUB, emb), jnp.float32)],
        cost_estimate=pl.CostEstimate(flops=20_000_000_000, bytes_accessed=13_000_000, transcendentals=0),
        name="compact_rows",
    )(starts[half::2], lens, by_table)


def ids_kernel(n_rows, ids_ref, len_ref, out_ref):
    shape = ids_ref.shape
    lane = lax.broadcasted_iota(jnp.int32, shape, 1)
    valid = len_ref[...] > 0
    count = valid.astype(jnp.int32)
    step = 1
    while step < shape[1]:
        count = count + jnp.where(lane >= step, pltpu.roll(count, step, 1), 0)
        step *= 2
    shift = lane + 1 - count
    packed = jnp.where(valid, ids_ref[...] + shift * (2 * n_rows), -1)
    step = 1
    while step < shape[1]:
        bit = step * 2 * n_rows
        moves = (packed & bit) != 0
        stay = jnp.where(jnp.logical_and(packed >= 0, jnp.logical_not(moves)), packed, -1)
        go = jnp.where(jnp.logical_and(packed >= 0, moves), packed, -1)
        packed = jnp.maximum(stay, pltpu.roll(go, shape[1] - step, 1))
        step *= 2
    out_ref[...] = jnp.where(packed >= 0, packed & (2 * n_rows - 1), n_rows)


def compact_ids(ids, lens, n_rows):
    return pl.pallas_call(
        functools.partial(ids_kernel, n_rows),
        out_shape=jax.ShapeDtypeStruct(ids.shape, jnp.int32),
        cost_estimate=pl.CostEstimate(flops=5_000_000_000, bytes_accessed=1_000_000, transcendentals=0),
        name="compact_ids",
    )(ids, lens)


def update_rows(acc, rate, table_ref, accum_ref, new_table_ref, new_accum_ref):
    n_blk, width = accum_ref.shape[1:]
    eye = lax.broadcasted_iota(jnp.int32, (width, width), 0) == lax.broadcasted_iota(jnp.int32, (width, width), 1)

    def block(blk, carry):
        rows = pl.ds(pl.multiple_of(blk * width, width), width)
        grad = acc[0][rows, :]
        for copy in acc[1:]:
            grad = grad + copy[rows, :]
        mean = jnp.mean(grad * grad, axis=1, keepdims=True)
        old = jnp.sum(jnp.where(eye, accum_ref[0, pl.ds(blk, 1), :], 0.0), axis=1, keepdims=True)
        new = old + mean
        scale = rate / (jnp.sqrt(new) + EPSILON)
        new_table_ref[0, rows, :] = (table_ref[0, rows, :].astype(jnp.float32) - grad * scale).astype(jnp.bfloat16)
        new_accum_ref[0, pl.ds(blk, 1), :] = jnp.sum(jnp.where(eye, new, 0.0), axis=0, keepdims=True)
        return carry

    lax.fori_loop(0, n_blk, block, 0)


def scatter_kernel(half, rate_ref, count_ref, ids_ref, recv_ref, table_ref, accum_ref, *rest):
    new_table_ref, new_accum_ref, rows_ref = rest[-(COPIES + 3) : -COPIES]
    acc = rest[-COPIES:]
    part = pl.program_id(0)

    @pl.when(part == 0)
    def _():
        for copy in acc:
            copy[...] = jnp.zeros_like(copy)

    rows_ref[...] = recv_ref[0].astype(jnp.float32)

    def step(i, carry):
        for group in range(0, ROWS, COPIES):
            base = i * ROWS + group
            where = [ids_ref[part, base + k] for k in range(COPIES)]
            total = [acc[k][pl.ds(where[k], 1), :] + rows_ref[pl.ds(base + k, 1), :] for k in range(COPIES)]
            for k in range(COPIES):
                acc[k][pl.ds(where[k], 1), :] = total[k]
        return carry

    lax.fori_loop(0, (count_ref[half, part] + (ROWS - 1)) // ROWS, step, 0)

    @pl.when(part == pl.num_programs(0) - 1)
    def _():
        update_rows(acc, rate_ref[0], table_ref, accum_ref, new_table_ref, new_accum_ref)


def scatter_update(half, recv, ids, counts, tables, accum, rate, earlier):
    n_group, cap, emb = recv.shape
    n_rows = tables.shape[1]
    slot = lambda i: (half, 0, 0)
    in_specs = [
        pl.BlockSpec(memory_space=pltpu.SMEM),
        pl.BlockSpec(memory_space=pltpu.SMEM),
        pl.BlockSpec((None,) + ids.shape[1:], slot, memory_space=pltpu.SMEM),
        pl.BlockSpec((1, cap, emb), lambda i: (i, 0, 0)),
        pl.BlockSpec((1, n_rows, emb), slot),
        pl.BlockSpec((1,) + accum.shape[1:], slot),
    ]
    args = [rate, counts, ids, recv, tables, accum]
    aliases = {}
    if earlier is not None:
        in_specs += [pl.BlockSpec(memory_space=pl.ANY)] * 2
        aliases = {len(args): 0, len(args) + 1: 1}
        args += list(earlier)
    return pl.pallas_call(
        functools.partial(scatter_kernel, half),
        grid=(n_group,),
        in_specs=in_specs,
        out_specs=[
            pl.BlockSpec((1, n_rows, emb), slot),
            pl.BlockSpec((1,) + accum.shape[1:], slot),
        ],
        out_shape=[jax.ShapeDtypeStruct(tables.shape, tables.dtype), jax.ShapeDtypeStruct(accum.shape, accum.dtype)],
        scratch_shapes=[pltpu.VMEM((cap, emb), jnp.float32)] + [pltpu.VMEM((n_rows + 8, emb), jnp.float32)] * COPIES,
        input_output_aliases=aliases,
        cost_estimate=pl.CostEstimate(flops=50_000_000_000, bytes_accessed=13_000_000, transcendentals=0),
        compiler_params=pltpu.CompilerParams(vmem_limit_bytes=60 * 1024 * 1024),
        name="scatter_update",
    )(*args)


def solution(mesh):
    n_group = mesh.shape['mp']
    slot_spec = P(('pod', 'mp'))

    def local_step(d_pool, row_ids, lengths, tables, row_accum, learn_rate):
        batch, n_tab, emb = d_pool.shape
        slots_dev, n_rows = tables.shape[:2]
        lanes = 128
        cap_fast = batch * 9 // 16

        by_source = (lengths > 0).reshape(slots_dev, n_group, batch)
        counts = jnp.sum(by_source, axis=2, dtype=jnp.int32)
        over = jnp.any(counts > cap_fast).astype(jnp.bfloat16)
        held = jnp.swapaxes(by_source, 0, 1).astype(jnp.bfloat16).reshape(n_group, -1, lanes)
        held = jnp.concatenate([held, jnp.full((n_group, 8, lanes), over)], axis=1)
        told = lax.all_to_all(held, 'mp', 0, 0, tiled=True)
        over_any = jnp.max(told[:, -1, 0]) > 0
        lens = told[:, :-8].astype(jnp.float32).reshape(n_group * slots_dev, batch // SUB, SUB)
        sub_counts = jnp.sum(lens, axis=2).astype(jnp.int32)
        starts = jnp.cumsum(sub_counts, axis=1) - sub_counts

        by_table = jnp.swapaxes(d_pool, 0, 1)
        seg_ids = row_ids.reshape(slots_dev * n_group, batch)
        ids = compact_ids(seg_ids, lengths.reshape(slots_dev * n_group, batch), n_rows)
        ids = ids.reshape(slots_dev, n_group, batch)
        accum = row_accum.reshape(slots_dev, n_rows // lanes, lanes)
        rate = learn_rate.reshape(1)

        def exchange(cap):
            done = None
            recvs = []
            for half in range(slots_dev):
                send = compact_rows(by_table, lens, starts, half, cap, n_group)
                recvs.append(lax.all_to_all(send, 'mp', 0, 0, tiled=True))
            for half in range(slots_dev):
                done = scatter_update(half, recvs[half], ids, counts, tables, accum, rate, done)
            return tuple(done)

        new_tables, new_accum = lax.cond(over_any, lambda: exchange(batch), lambda: exchange(cap_fast))
        return new_tables, new_accum.reshape(row_accum.shape)

    return jax.shard_map(local_step, mesh=mesh, in_specs=(slot_spec, slot_spec, slot_spec, slot_spec, slot_spec, P()), out_specs=(slot_spec, slot_spec), check_vma=False)
```
